16 devices in a mesh: dp: 4 (over y, z, core), tp: 4 (over x).
Axes of the slice: x: 4, y: 2, z: 1, core: 2. Of those that a mesh axis runs over, the one named last changes fastest.
The devices are a block of a 4x4x8 slice.
Arguments:
- x: bfloat16 [16, 512, 4608], P('dp'), parts along dimension 0
- gain_a: bfloat16 [4608], replicated
- wq: bfloat16 [4608, 4096], P(None, 'tp')
- wk: bfloat16 [4608, 2048], P(None, 'tp')
- wv: bfloat16 [4608, 2048], P(None, 'tp')
- wo: bfloat16 [4096, 4608], P('tp')
- gain_m: bfloat16 [4608], replicated
- w_gate: bfloat16 [4608, 36864], P(None, 'tp')
- w_up: bfloat16 [4608, 36864], P(None, 'tp')
- w_down: bfloat16 [36864, 4608], P('tp')
Outputs:
- output: bfloat16 [16, 512, 4608], P('dp'), parts along dimension 0
There are 4 independent parts. The reference program is written for one: setup_inputs(seed, part) draws one part's arguments, and reference() takes and returns one part's arrays. A program takes and returns all parts, laid end to end along the dimension named above; an argument that names none is the same for every part.
All inputs are finite; a program needn't handle non-finite values.
Results may differ from the reference program's by a relative error of at most 0.017.
Values are sent between devices in bfloat16 or wider.
A program may use at most 768 MiB of HBM per device.

```python
import jax
import jax.numpy as jnp
from jax import lax

SEQUENCES = 4
TOKENS = 512
D = 4608
HEADS = 32
KV_HEADS = 16
HEAD = 128
FF = 36864
THETA = 10000


def setup_inputs(seed: int = 0, part: int = 0) -> dict:
    kx, ka, km, kq, kk, kv, ko, kg, ku, kd = jax.random.split(jax.random.key(seed), 10)

    def weights(key, rows, columns):
        return jax.random.normal(key, (rows, columns), jnp.float32) * rows**-0.5

    drawn = {
        "x": jax.random.normal(jax.random.fold_in(kx, part), (SEQUENCES, TOKENS, D), jnp.float32),
        "gain_a": 1 + 0.1 * jax.random.normal(ka, (D,), jnp.float32),
        "wq": 2 * weights(kq, D, HEADS * HEAD),
        "wk": 2 * weights(kk, D, KV_HEADS * HEAD),
        "wv": 4 * weights(kv, D, KV_HEADS * HEAD),
        "wo": weights(ko, HEADS * HEAD, D),
        "gain_m": 1 + 0.1 * jax.random.normal(km, (D,), jnp.float32),
        "w_gate": weights(kg, D, FF),
        "w_up": weights(ku, D, FF),
        "w_down": 3 * weights(kd, FF, D),
    }
    return {k: v.astype(jnp.bfloat16) for k, v in drawn.items()}


def normed(x, gain):
    wide = x.astype(jnp.float32)
    scale = lax.rsqrt(jnp.mean(wide * wide, -1, keepdims=True) + 1e-6)
    return (wide * scale * gain.astype(jnp.float32)).astype(jnp.bfloat16)


def turned(t, place, theta):
    half = t.shape[-1] // 2
    angle = place.astype(jnp.float32)[:, None] * theta ** (-jnp.arange(half, dtype=jnp.float32) / half)
    cos, sin = jnp.cos(angle)[:, None], jnp.sin(angle)[:, None]
    a, b = t[..., :half].astype(jnp.float32), t[..., half:].astype(jnp.float32)
    return jnp.concatenate([a * cos - b * sin, b * cos + a * sin], -1).astype(jnp.bfloat16)


def matmul(a, w):
    return jnp.dot(a, w, preferred_element_type=jnp.float32).astype(jnp.bfloat16)


def einsum(form, a, b):
    return jnp.einsum(form, a.astype(jnp.float32), b.astype(jnp.float32))


def attention(q, k, v):
    scores = einsum("tgsd,ugd->gstu", q, k) * q.shape[-1] ** -0.5
    token = jnp.arange(q.shape[0])
    scores = jnp.where(token[:, None] >= token, scores, -jnp.inf)
    weights = jax.nn.softmax(scores, -1).astype(jnp.bfloat16)
    return einsum("gstu,ugd->tgsd", weights, v).astype(jnp.bfloat16)


def one(x, gain_a, wq, wk, wv, wo, gain_m, w_gate, w_up, w_down):
    rows = x.shape[0]
    a, place = normed(x, gain_a), jnp.arange(rows)
    k = turned(matmul(a, wk).reshape(rows, -1, HEAD), place, THETA)
    q = turned(matmul(a, wq).reshape(rows, -1, HEAD), place, THETA).reshape(rows, k.shape[1], -1, HEAD)
    v = matmul(a, wv).reshape(rows, -1, HEAD)
    seen = attention(q, k, v).reshape(rows, -1)
    h = (x.astype(jnp.float32) + jnp.dot(seen, wo, preferred_element_type=jnp.float32)).astype(jnp.bfloat16)
    b = normed(h, gain_m)
    gate = jnp.dot(b, w_gate, preferred_element_type=jnp.float32)
    up = jnp.dot(b, w_up, preferred_element_type=jnp.float32)
    hidden = (jax.nn.silu(gate) * up).astype(jnp.bfloat16)
    return (h.astype(jnp.float32) + jnp.dot(hidden, w_down, preferred_element_type=jnp.float32)).astype(jnp.bfloat16)


def reference(x, gain_a, wq, wk, wv, wo, gain_m, w_gate, w_up, w_down):
    return lax.map(lambda sequence: one(sequence, gain_a, wq, wk, wv, wo, gain_m, w_gate, w_up, w_down), x)
```

```python
import functools

import jax
import jax.numpy as jnp
from jax import lax
from jax.experimental import pallas as pl
from jax.experimental.pallas import tpu as pltpu
from jax.sharding import PartitionSpec as P

HEAD = 128
THETA = 10000
HIDDEN = -2e30
LOG2E = 1.4426950408889634
TILE = 256
UNIT = 2 * TILE
LAG2, LAG3 = 3, 5
MESH = pl.DeviceIdType.MESH
F32, BF16 = jnp.float32, jnp.bfloat16


def dot(a, b):
    return jnp.dot(a, b, preferred_element_type=F32)


def layer_kernel(seqs, pieces, x, cos, sin, gain_a, gain_m, wq, wk, wv, wo, wg, wu, wd, y, hb,
                 b, hid, slot, seen, out, own, rel, send1, send2, recv1, recv2, rblk, wob,
                 wsem, wosem, wobsem, xsem, bsem, xbsem, s1s, s1r, s2s, s2r, credit, ysem, bstsem,
                 ha1s, ha1r, ha2s, ha2r, ya1s, ya1r, ya2s, ya2r):
    m, d = b.shape
    f = hid.shape[1]
    n = lax.axis_size("tp")
    blk = m // 4
    nu, ng = d // UNIT, f // UNIT
    per = ng + nu
    last = seqs - 1
    hq = wq.shape[1]
    wide = d // pieces
    me = lax.axis_index("tp")
    right, left, far = lax.rem(me + 1, n), lax.rem(me + n - 1, n), lax.rem(me + 2, n)

    def rows(chunk, block, size=None, at=0):
        return pl.ds(pl.multiple_of(chunk * m + block * blk + at, 16 if size is None else 8), size or blk)

    def cols(j, width=UNIT):
        return pl.ds(pl.multiple_of(j * width, 128), width)

    def remote(src, dst, send, recv, to):
        return pltpu.make_async_remote_copy(src, dst, send, recv, device_id={"tp": to}, device_id_type=MESH)

    copy = pltpu.make_async_copy

    def qkv_tiles(i, p):
        w, c = ((wq, 0), (wq, UNIT), (wk, 0), (wv, 0))[i]
        return [copy(w.at[:, pl.ds(c + u * TILE, TILE)], slot.at[p, u, pl.ds(0, d)], wsem.at[p, u]) for u in range(2)]

    def wo_tiles(p):
        return [copy(wo.at[:, pl.ds(j * UNIT + u * TILE, TILE)], slot.at[p, u, pl.ds(j * hq, hq)], wosem.at[2 * j + u])
                for j in range(nu) for u in range(2)]

    def gu_tiles(k, p):
        return [copy(w.at[:, pl.ds(pl.multiple_of(k * UNIT + u * TILE, TILE), TILE)], slot.at[p, u, pl.ds(h * d, d)], wsem.at[p, 2 * u + h])
                for u in range(2) for h, w in enumerate((wg, wu))]

    def dn_tiles(k, p):
        return [copy(wd.at[:, pl.ds(pl.multiple_of(k * UNIT + u * TILE, TILE), TILE)], slot.at[p, u], wsem.at[p, u]) for u in range(2)]

    def start(copies):
        for c in copies:
            c.start()

    def wait(copies):
        for c in copies:
            c.wait()

    def wo_unit(j):
        return copy(wo.at[:, cols(j)], wob, wobsem)

    def stage1(j, par):
        at = lambda block: pl.ds(pl.multiple_of(block * blk, 16), blk)
        lo, hi = slice(0, TILE), slice(TILE, UNIT)
        send1[0, j, 0] = out[par, at(far), lo].astype(BF16)
        send1[1, j, 0] = out[par, at(far), hi].astype(BF16)
        send1[0, j, 1] = out[par, at(right), hi].astype(BF16)
        send1[1, j, 1] = out[par, at(left), lo].astype(BF16)
        rel[0, j] = out[par, at(right), lo]
        rel[1, j] = out[par, at(left), hi]
        own[j] = out[par, at(me), :]

    def stage2(j):
        for way in range(2):
            send2[way, j] = (rel[way, j] + recv1[way, j, 0].astype(F32)).astype(BF16)

    def stage3(j, res, dst):
        base = pl.multiple_of(j * UNIT, UNIT)
        for h in range(2):
            c = pl.ds(base + h * TILE, TILE)
            total = own[j, :, h * TILE : (h + 1) * TILE] + recv2[h, j].astype(F32) + recv1[1 - h, j, 1].astype(F32)
            rblk[dst, :, c] = (rblk[res, :, c].astype(F32) + total).astype(BF16)

    def rs1(j):
        return [remote(send1.at[w, j], recv1.at[w, j], s1s.at[w, j], s1r.at[w, j], to) for w, to in enumerate((right, left))]

    def rs2(j):
        return [remote(send2.at[w, j], recv2.at[w, j], s2s.at[w, j], s2r.at[w, j], to) for w, to in enumerate((right, left))]

    def received(copies):
        for c in copies:
            c.wait_recv()

    def sent(copies):
        for c in copies:
            c.wait_send()

    def give_credit(j):
        for w, to in enumerate((left, right)):
            pl.semaphore_signal(credit.at[w, j], inc=1, device_id={"tp": to}, device_id_type=MESH)

    def take_credit(j):
        for w in range(2):
            pl.semaphore_wait(credit.at[w, j], 1)

    def y_block(c, j):
        return copy(rblk.at[3, :, cols(j)], y.at[rows(c, me), cols(j)], ysem.at[j])

    def x_block(c):
        return copy(x.at[rows(c, me)], rblk.at[2, :, pl.ds(0, d)], xbsem)

    def gather1(buf, c, p, s, r, src=None):
        a = buf.at[rows(c, me), cols(p, wide)]
        src = a if src is None else src.at[:, cols(p, wide)]
        return [remote(src, a, s.at[w, p], r.at[w, p], to) for w, to in enumerate((right, left))]

    def gather2(buf, c, p, s, r):
        half = blk // 2
        a = [buf.at[rows(c, left, half), cols(p, wide)], buf.at[rows(c, right, half, half), cols(p, wide)]]
        return [remote(a[w], a[w], s.at[w, p], r.at[w, p], to) for w, to in enumerate((right, left))]

    bst = rblk.at[3, :, pl.ds(0, d)]

    def h_gather1(c):
        return [g for p in range(pieces) for g in gather1(hb, c, p, ha1s, ha1r, bst)]

    def h_gather2(c):
        return [g for p in range(pieces) for g in gather2(hb, c, p, ha2s, ha2r)]

    def b_own(c):
        return copy(bst, hb.at[rows(c, me)], bstsem)

    def norm_rows(src, gain, dst, count):
        @pl.loop(0, count // 16)
        def _(i):
            r = pl.ds(pl.multiple_of(i * 16, 16), 16)
            w = src[r, :].astype(F32)
            scale = lax.rsqrt(jnp.mean(w * w, -1, keepdims=True) + 1e-6)
            dst[r, :] = (w * scale * gain[...].astype(F32)).astype(BF16)

    def h_norm(c):
        norm_rows(rblk.at[lax.rem(c, 2), :, pl.ds(0, d)], gain_m, bst, blk)
        b_own(c).start()
        start(h_gather1(c))

    def h_forward(c, p):
        received(gather1(hb, c, p, ha1s, ha1r))
        start(gather2(hb, c, p, ha2s, ha2r))

    def b_load(c):
        return copy(hb.at[pl.ds(pl.multiple_of(c * m, 16), m)], b, bsem)

    def x_load(s):
        return copy(x.at[pl.ds(pl.multiple_of(s * m, 16), m)], hid.at[:, pl.ds(0, d)], xsem)

    def project(i, p):
        plain = i == 3
        c, s = jnp.where(plain, 1.0, cos[...]), jnp.where(plain, 0.0, sin[...])
        for u in range(2):
            r = dot(b[...], slot[p, u, :d])
            for h in range(TILE // HEAD):
                t = r[:, h * HEAD : (h + 1) * HEAD].astype(BF16).astype(F32)
                o = t * c + pltpu.roll(t, HEAD // 2, 1) * s
                hid[:, pl.ds(pl.multiple_of(d + i * UNIT + u * TILE + h * HEAD, HEAD), HEAD)] = o.astype(BF16)

    def heads(s, g):
        e = HEAD**-0.5 * LOG2E
        half = m // 2
        at = lambda c: pl.ds(pl.multiple_of(d + c, HEAD), HEAD)
        for qb in range(2):
            keys, these = (qb + 1) * half, pl.ds(qb * half, half)
            kk, vv = hid[0:keys, at(2 * UNIT + g * HEAD)], hid[0:keys, at(3 * UNIT + g * HEAD)]
            q = jnp.concatenate([hid[these, at(2 * g * HEAD)], hid[these, at((2 * g + 1) * HEAD)]], axis=0)
            sc = lax.dot_general(kk, q, (((1,), (1,)), ((), ())), preferred_element_type=F32)
            ok = lax.broadcasted_iota(jnp.int32, (half, 2 * half), 0) <= lax.rem(lax.broadcasted_iota(jnp.int32, (half, 2 * half), 1), half)
            cut = jnp.where(ok, sc[qb * half :], HIDDEN)
            sc = cut if qb == 0 else jnp.concatenate([sc[:half], cut], axis=0)
            w = jnp.exp2((sc - sc.max(axis=0, keepdims=True)) * e).astype(BF16)
            mix = dot(jnp.concatenate([vv.T, jnp.ones((8, keys), BF16)], axis=0), w)
            o = (mix[:HEAD] * (1 / mix[HEAD : HEAD + 1])).T.astype(BF16)
            to = pl.ds(pl.multiple_of(s * m + qb * half, 16), half)
            for h in range(2):
                seen[to, pl.ds(pl.multiple_of((2 * g + h) * HEAD, HEAD), HEAD)] = o[h * half : (h + 1) * half]

    def first_service(k):
        @pl.when((k >= 2) & (k < 2 + nu))
        def _():
            j = k - 2
            received(rs1(j))
            stage2(j)
            start(rs2(j))

        @pl.when((k >= 4 + nu) & (k < 4 + 2 * nu))
        def _():
            j = k - 4 - nu
            received(rs2(j))
            sent(rs1(j) + rs2(j))
            stage3(j, 2, 0)
            give_credit(j)

        @pl.when(k == 4 + 2 * nu)
        def _():
            h_norm(0)

    def attention(s, first):
        x_load(s).wait()
        norm_rows(hid.at[:, pl.ds(0, d)], gain_a, b, m)

        @pl.when(s < last)
        def _():
            x_load(s + 1).start()

        @pl.loop(0, 4)
        def _(i):
            p = lax.rem(i, 2) if first else lax.rem(i + 1, 2)
            wait(qkv_tiles(0, p))
            for nxt in range(1, 4):
                @pl.when(i == nxt - 1)
                def _():
                    start(qkv_tiles(nxt, 1 - p))

            @pl.when(i == 3)
            def _():
                if first:
                    start(wo_tiles(1 - p))
                else:
                    @pl.when(s < last)
                    def _():
                        start(qkv_tiles(0, 1 - p))

                    @pl.when(s == last)
                    def _():
                        start(gu_tiles(0, 1 - p))
            if not first:
                first_service(8 * (s - 1) + i)
            project(i, p)

        @pl.loop(0, 4)
        def _(g):
            if not first:
                first_service(8 * (s - 1) + 4 + g)
            heads(s, g)

    barrier = pltpu.get_barrier_semaphore()
    for to in (left, right):
        pl.semaphore_signal(barrier, inc=1, device_id={"tp": to}, device_id_type=MESH)
    x_load(0).start()
    start(qkv_tiles(0, 0))
    x_block(0).start()
    pl.semaphore_wait(barrier, 2)

    attention(0, True)
    wait(wo_tiles(0))
    start(qkv_tiles(0, 1))
    x_block(0).wait()

    @pl.loop(0, nu)
    def _(j):
        par = lax.rem(j, 2)
        for u in range(2):
            tile = slot[0, u, pl.ds(pl.multiple_of(j * hq, hq), hq), :]
            out[par, :, u * TILE : (u + 1) * TILE] = dot(seen[0:m, :], tile)
        stage1(j, par)
        start(rs1(j))

    @pl.loop(1, seqs)
    def _(s):
        attention(s, False)

    for p in range(pieces):
        h_forward(0, p)
    wo_unit(0).start()
    sent(h_gather1(0))
    b_own(0).wait()
    received(h_gather2(0))
    sent(h_gather2(0))
    b_load(0).start()

    def unit(t):
        past = t >= 0
        t = jnp.maximum(t, 0)
        c, k = lax.div(t, per), lax.rem(t, per)
        second = k >= ng
        there = past & (c <= last) & (second | ((k < nu) & (c < last)))
        return there, second, c, jnp.where(second, k - ng, k)

    def place(there, j):
        return jnp.where(there, j, nu)

    when = y_schedule(seqs, pieces, ng)

    def before(c, k, t):
        u2, u3 = unit(t - LAG2), unit(t - LAG3)

        @pl.when(u2[0])
        def _():
            received(rs1(u2[3]))

        @pl.when(u3[0] & jnp.logical_not(u3[1]) & (u3[3] == 0))
        def _():
            x_block(0).wait()

        @pl.when(u3[0])
        def _():
            received(rs2(u3[3]))
            sent(rs1(u3[3]) + rs2(u3[3]))

    def math(t):
        u1, u2, u3 = unit(t - 1), unit(t - LAG2), unit(t - LAG3)
        stage1(place(u1[0], u1[3]), lax.rem(t + 1, 2))
        stage2(place(u2[0], u2[3]))
        of_y = u3[1]
        stage3(place(u3[0], u3[3]), jnp.where(of_y, lax.rem(u3[2], 2), 2), jnp.where(of_y, 3, lax.rem(u3[2] + 1, 2)))

    def after(c, k, t):
        u1, u2, u3 = unit(t - 1), unit(t - LAG2), unit(t - LAG3)

        @pl.when(u1[0])
        def _():
            take_credit(u1[3])
            start(rs1(u1[3]))

        @pl.when(u2[0])
        def _():
            start(rs2(u2[3]))

        @pl.when(u3[0])
        def _():
            give_credit(u3[3])

        @pl.when(u3[0] & u3[1])
        def _():
            y_block(u3[2], u3[3]).start()

    def gathers(c, k, low, high):
        def at(tick, cond=True):
            return pl.when((k == tick) & cond) if low <= tick < high else lambda f: None

        more = c < last

        @at(0, more)
        def _():
            x_block(c + 1).start()

        @at(6, c > 0)
        def _():
            for j in range(nu):
                y_block(c - 1, j).wait()

        normed_at = LAG3 + nu
        @at(normed_at, more)
        def _():
            h_norm(c + 1)

        for p in range(pieces):
            @at(normed_at + (3, 5, 6)[p], more)
            def _():
                h_forward(c + 1, p)

        @at(normed_at + 7, more)
        def _():
            sent(h_gather1(c + 1))
            b_own(c + 1).wait()

        @at(per - 2, more)
        def _():
            received(h_gather2(c + 1))
            sent(h_gather2(c + 1))
            b_load(c + 1).start()

        @at(per - 2, c + 1 < last)
        def _():
            wo_unit(0).start()

        for (cy, p), ((c1, k1), (c2, k2)) in when.items():
            @at(k1, c == c1)
            def _():
                start(gather1(y, cy, p, ya1s.at[cy], ya1r.at[cy]))

            @at(k2, c == c2)
            def _():
                received(gather1(y, cy, p, ya1s.at[cy], ya1r.at[cy]))
                start(gather2(y, cy, p, ya2s.at[cy], ya2r.at[cy]))

    first_item = 4 * seqs + 1

    @pl.loop(0, seqs)
    def _(c):
        b_load(c).wait()

        @pl.loop(0, ng)
        def _(k):
            t = c * per + k
            p = lax.rem(first_item + t, 2)
            wait(gu_tiles(0, p))

            @pl.when(k < ng - 1)
            def _():
                start(gu_tiles(k + 1, 1 - p))

            @pl.when(k == ng - 1)
            def _():
                start(dn_tiles(0, 1 - p))

            @pl.when((k < nu) & (c < last))
            def _():
                wo_unit(0).wait()
                out[lax.rem(t, 2)] = dot(seen[pl.ds(pl.multiple_of((c + 1) * m, 16), m), :], wob[...])

                @pl.when(k < nu - 1)
                def _():
                    wo_unit(k + 1).start()

            before(c, k, t)
            for u in range(2):
                gate, up = dot(b[...], slot[p, u, :d]), dot(b[...], slot[p, u, d:])
                hid[:, pl.ds(pl.multiple_of(k * UNIT + u * TILE, TILE), TILE)] = (gate * jax.nn.sigmoid(gate) * up).astype(BF16)
            math(t)
            after(c, k, t)
            gathers(c, k, 0, ng)

        @pl.loop(0, nu)
        def _(j):
            k = ng + j
            t = c * per + k
            p = lax.rem(first_item + t, 2)
            wait(dn_tiles(0, p))

            @pl.when(j < nu - 1)
            def _():
                start(dn_tiles(j + 1, 1 - p))

            @pl.when((j == nu - 1) & (c < last))
            def _():
                start(gu_tiles(0, 1 - p))

            before(c, k, t)
            for u in range(2):
                out[lax.rem(t, 2), :, u * TILE : (u + 1) * TILE] = dot(hid[...], slot[p, u])
            math(t)
            after(c, k, t)
            gathers(c, k, ng, per)

    done, piece = 0, 0
    end = seqs * per
    def finish_pieces():
        nonlocal piece
        while piece < pieces and done >= (piece + 1) * nu // pieces:
            start(gather1(y, last, piece, ya1s.at[last], ya1r.at[last], rblk.at[3, :, pl.ds(0, d)]))
            piece += 1

    done = nu - LAG3
    for dt in range(LAG3):
        if dt == 0:
            stage1(nu - 1, (end + 1) % 2)
            take_credit(nu - 1)
            start(rs1(nu - 1))
            finish_pieces()
        j2, j3 = nu + dt - LAG2, nu + dt - LAG3
        if j2 < nu:
            received(rs1(j2))
            stage2(j2)
            start(rs2(j2))
        received(rs2(j3))
        sent(rs1(j3) + rs2(j3))
        stage3(j3, last % 2, 3)
        give_credit(j3)
        y_block(last, j3).start()
        done = j3 + 1
        finish_pieces()
    for p in range(pieces):
        received(gather1(y, last, p, ya1s.at[last], ya1r.at[last]))
        start(gather2(y, last, p, ya2s.at[last], ya2r.at[last]))
    for j in range(nu):
        y_block(last, j).wait()
        take_credit(j)
    for c in range(seqs):
        for p in range(pieces):
            one, two = gather1(y, c, p, ya1s.at[c], ya1r.at[c]), gather2(y, c, p, ya2s.at[c], ya2r.at[c])
            sent(one + two)
            received(two)


def y_schedule(seqs, pieces, ng):
    when = {}
    last = seqs - 1
    when[0, 0] = (1, 11), (1, 15)
    when[0, 1] = (2, 11), (2, 15)
    when[0, 2] = (3, 0), (3, 3)
    for p in range(3):
        when[1, p] = (3, p), (3, (5, 7, 8)[p])
    for p in range(3):
        when[2, p] = (3, (9, 9, 10)[p]), (3, (13, 15, 16)[p])
    return when


def rotary(rows):
    half = HEAD // 2
    angle = jnp.arange(rows, dtype=F32)[:, None] * THETA ** (-jnp.arange(half, dtype=F32) / half)
    cos, sin = jnp.cos(angle), jnp.sin(angle)
    return jnp.concatenate([cos, cos], -1), jnp.concatenate([-sin, sin], -1)


def solution(mesh):
    pieces = 3

    def step(x, gain_a, wq, wk, wv, wo, gain_m, w_gate, w_up, w_down):
        seqs, m, d = x.shape
        f, hq = w_gate.shape[1], wq.shape[1]
        blk, nu = m // 4, d // UNIT
        cos, sin = rotary(m)
        anywhere, vmem = pl.BlockSpec(memory_space=pl.ANY), pl.BlockSpec(memory_space=pltpu.VMEM)
        dma, V = pltpu.SemaphoreType.DMA, pltpu.VMEM
        y, _ = pl.pallas_call(
            functools.partial(layer_kernel, seqs, pieces),
            out_shape=[jax.ShapeDtypeStruct((seqs * m, d), BF16)] * 2,
            in_specs=[anywhere] + [vmem] * 4 + [anywhere] * 7,
            out_specs=[anywhere] * 2,
            scratch_shapes=[
                V((m, d), BF16), V((m, f), BF16), V((2, 2, 2 * d, TILE), BF16), V((seqs * m, hq), BF16), V((2, m, UNIT), F32),
                V((nu + 1, blk, UNIT), F32), V((2, nu + 1, blk, TILE), F32),
                V((2, nu + 1, 2, blk, TILE), BF16), V((2, nu + 1, blk, TILE), BF16),
                V((2, nu + 1, 2, blk, TILE), BF16), V((2, nu + 1, blk, TILE), BF16),
                V((4, blk, d + UNIT), BF16), V((hq, UNIT), BF16),
                dma((2, 4)), dma((2 * nu,)), dma, dma, dma, dma, dma((2, nu)), dma((2, nu)), dma((2, nu)), dma((2, nu)),
                pltpu.SemaphoreType.REGULAR((2, nu)), dma((nu,)), dma,
                dma((2, pieces)), dma((2, pieces)), dma((2, pieces)), dma((2, pieces)),
                dma((seqs, 2, pieces)), dma((seqs, 2, pieces)), dma((seqs, 2, pieces)), dma((seqs, 2, pieces)),
            ],
            compiler_params=pltpu.CompilerParams(collective_id=0, has_side_effects=True, vmem_limit_bytes=67043328),
            name="layer",
        )(x.reshape(seqs * m, d), cos, sin, gain_a.reshape(1, d), gain_m.reshape(1, d), wq, wk, wv, wo, w_gate, w_up, w_down)
        return y.reshape(x.shape)

    tokens, whole, columns, rows_of = P("dp", None, None), P(None), P(None, "tp"), P("tp", None)
    return jax.shard_map(
        step,
        mesh=mesh,
        in_specs=(tokens, whole, columns, columns, columns, rows_of, whole, columns, columns, rows_of),
        out_specs=tokens,
        check_vma=False,
    )
```

```python
import functools

import jax
import jax.numpy as jnp
import numpy as np
from jax import lax
from jax.experimental import pallas as pl
from jax.experimental.pallas import tpu as pltpu
from jax.sharding import PartitionSpec as P

HEAD = 128
THETA = 10000
HIDDEN = -2e30
LOG2E = 1.4426950408889634
TILE = 256
UNIT = 2 * TILE
TIMES = dict(w=4, relay=7, finish=9, norm=14, forward=(17, 18, 20))
FIRST = dict(relay=2, finish=9, norm=14, forward=(17, 19, 21))
LAGS, LAST_LAGS = (4, 7), (2, 4)
GATHER = ((12, 3), (24, 3), (9, 1))
GATHER_LAG = 5
SEGMENTS = ((0, 9, (2, 2, 1)), (9, 14, (0, 2, 2)), (14, None, (0, 0, 0)))
RELAYED = {0: (0, 1), 1: (2,), 2: (3,), 3: (4,), 4: (5,), 6: (6,), 8: (7, 8)}
FINISHED = {9: (0,), 10: (1, 2), 11: (3, 4), 12: (5, 6), 13: (7,), 14: (8,)}
NORMED = 15
MESH = pl.DeviceIdType.MESH
F32, BF16 = jnp.float32, jnp.bfloat16


def dot(a, b):
    return jnp.dot(a, b, preferred_element_type=F32)


def layer_kernel(seqs, pieces, x, cos, sin, gains, wq, wk, wv, wo, wg, wu, wd, y, hb,
                 b, hid, slot, seen, out, own, rel, send1, send2, recv1, recv2, rblk, wob,
                 wsem, wobsem, xsem, bsem, xbsem, s1s, s1r, s2s, s2r, credit, ysem, bstsem,
                 ha1s, ha1r, ha2s, ha2r, ya1s, ya1r, ya2s, ya2r):
    m, d = b.shape
    f = hid.shape[1]
    n = lax.axis_size("tp")
    blk = m // 4
    nu, ng = d // UNIT, f // UNIT
    per = ng + nu
    last = seqs - 1
    hq = wq.shape[1]
    wide = d // pieces
    me = lax.axis_index("tp")
    right, left, far = lax.rem(me + 1, n), lax.rem(me + n - 1, n), lax.rem(me + 2, n)

    def rows(chunk, block, size=None, at=0):
        return pl.ds(pl.multiple_of(chunk * m + block * blk + at, 16 if size is None else 8), size or blk)

    def cols(j, width=UNIT):
        return pl.ds(pl.multiple_of(j * width, 128), width)

    def remote(src, dst, send, recv, to):
        return pltpu.make_async_remote_copy(src, dst, send, recv, device_id={"tp": to}, device_id_type=MESH)

    copy = pltpu.make_async_copy

    def qkv_tiles(i):
        w, c = ((wq, 0), (wq, UNIT), (wk, 0), (wv, 0))[i]
        p, h = i % 2, i // 2
        return [copy(w.at[:, pl.ds(c + u * TILE, TILE)], slot.at[p, u, pl.ds(h * d, d)], wsem.at[p, 2 * u + h]) for u in range(2)]

    def gu_tiles(k, p):
        return [copy(w.at[:, pl.ds(pl.multiple_of(k * UNIT + u * TILE, TILE), TILE)], slot.at[p, u, pl.ds(h * d, d)], wsem.at[p, 2 * u + h])
                for u in range(2) for h, w in enumerate((wg, wu))]

    def dn_tiles(k, p):
        return [copy(wd.at[:, pl.ds(pl.multiple_of(k * UNIT + u * TILE, TILE), TILE)], slot.at[p, u], wsem.at[p, u]) for u in range(2)]

    def start(copies):
        for c in copies:
            c.start()

    def wait(copies):
        for c in copies:
            c.wait()

    def wo_unit(j):
        return copy(wo.at[:, cols(j)], wob.at[lax.rem(j, 2)], wobsem.at[lax.rem(j, 2)])

    def stage1(j, par):
        at = lambda block: pl.ds(pl.multiple_of(block * blk, 16), blk)
        lo, hi = slice(0, TILE), slice(TILE, UNIT)
        send1[0, j, 0] = out[par, at(far), lo].astype(BF16)
        send1[1, j, 0] = out[par, at(far), hi].astype(BF16)
        send1[0, j, 1] = out[par, at(right), hi].astype(BF16)
        send1[1, j, 1] = out[par, at(left), lo].astype(BF16)
        rel[0, j] = out[par, at(right), lo]
        rel[1, j] = out[par, at(left), hi]
        own[j] = out[par, at(me), :]

    def stage2(j):
        for way in range(2):
            send2[way, j] = (rel[way, j] + recv1[way, j, 0].astype(F32)).astype(BF16)

    def stage3(j, res, dst):
        base = pl.multiple_of(j * UNIT, UNIT)
        for h in range(2):
            c = pl.ds(base + h * TILE, TILE)
            total = own[j, :, h * TILE : (h + 1) * TILE] + recv2[h, j].astype(F32) + recv1[1 - h, j, 1].astype(F32)
            rblk[dst, :, c] = (rblk[res, :, c].astype(F32) + total).astype(BF16)

    def rs1(j):
        return [remote(send1.at[w, j], recv1.at[w, j], s1s.at[w, j], s1r.at[w, j], to) for w, to in enumerate((right, left))]

    def rs2(j):
        return [remote(send2.at[w, j], recv2.at[w, j], s2s.at[w, j], s2r.at[w, j], to) for w, to in enumerate((right, left))]

    def received(copies):
        for c in copies:
            c.wait_recv()

    def sent(copies):
        for c in copies:
            c.wait_send()

    def give_credit(j):
        for w, to in enumerate((left, right)):
            pl.semaphore_signal(credit.at[w, j], inc=1, device_id={"tp": to}, device_id_type=MESH)

    def take_credit(j):
        for w in range(2):
            pl.semaphore_wait(credit.at[w, j], 1)

    def y_gather1(c, j, src=None):
        a = y.at[rows(c, me), cols(j)]
        src = a if src is None else src.at[:, cols(j)]
        return [remote(src, a, ya1s.at[c, w, j], ya1r.at[c, w, j], to) for w, to in enumerate((right, left))]

    def y_gather2(c, j):
        half = blk // 2
        a = [y.at[rows(c, left, half), cols(j)], y.at[rows(c, right, half, half), cols(j)]]
        return [remote(a[w], a[w], ya2s.at[c, w, j], ya2r.at[c, w, j], to) for w, to in enumerate((right, left))]

    def y_block(c, j):
        return copy(rblk.at[3, :, cols(j)], y.at[rows(c, me), cols(j)], ysem.at[j])

    def x_block(c):
        return copy(x.at[rows(c, me)], rblk.at[2, :, pl.ds(0, d)], xbsem)

    def gather1(buf, c, p, s, r, src=None):
        a = buf.at[rows(c, me), cols(p, wide)]
        src = a if src is None else src.at[:, cols(p, wide)]
        return [remote(src, a, s.at[w, p], r.at[w, p], to) for w, to in enumerate((right, left))]

    def gather2(buf, c, p, s, r):
        half = blk // 2
        a = [buf.at[rows(c, left, half), cols(p, wide)], buf.at[rows(c, right, half, half), cols(p, wide)]]
        return [remote(a[w], a[w], s.at[w, p], r.at[w, p], to) for w, to in enumerate((right, left))]

    bst = rblk.at[3, :, pl.ds(0, d)]

    def h_gather1(c):
        return [g for p in range(pieces) for g in gather1(hb, c, p, ha1s, ha1r, bst)]

    def h_gather2(c):
        return [g for p in range(pieces) for g in gather2(hb, c, p, ha2s, ha2r)]

    def b_own(c):
        return copy(bst, hb.at[rows(c, me)], bstsem)

    def norm_rows(src, gain, dst, count):
        together = min(4, count // 16)

        @pl.loop(0, count // (16 * together))
        def _(i):
            at = [pl.ds(pl.multiple_of((i * together + g) * 16, 16), 16) for g in range(together)]
            scales = []
            for r in at:
                w = src[r, :].astype(F32)
                scales.append(lax.rsqrt(jnp.mean(w * w, -1, keepdims=True) + 1e-6))
            for r, scale in zip(at, scales):
                dst[r, :] = (src[r, :].astype(F32) * scale * gain[...].astype(F32)).astype(BF16)

    def h_norm(c):
        norm_rows(rblk.at[lax.rem(c, 2), :, pl.ds(0, d)], gains.at[1:2], bst, blk)
        b_own(c).start()
        start(h_gather1(c))

    def h_forward(c, p):
        received(gather1(hb, c, p, ha1s, ha1r))
        start(gather2(hb, c, p, ha2s, ha2r))

    def b_load(c):
        return copy(hb.at[pl.ds(pl.multiple_of(c * m, 16), m)], b, bsem)

    def x_load(s):
        return copy(x.at[pl.ds(pl.multiple_of(s * m, 16), m)], hid.at[:, pl.ds(0, d)], xsem)

    def project(i):
        p, h = lax.rem(i, 2), lax.div(i, 2)
        plain = i == 3
        c, s = jnp.where(plain, 1.0, cos[...]), jnp.where(plain, 0.0, sin[...])
        for u in range(2):
            r = dot(b[...], slot[p, u, pl.ds(pl.multiple_of(h * d, d), d), :])
            for q in range(TILE // HEAD):
                t = r[:, q * HEAD : (q + 1) * HEAD].astype(BF16).astype(F32)
                o = t * c + pltpu.roll(t, HEAD // 2, 1) * s
                hid[:, pl.ds(pl.multiple_of(d + i * UNIT + u * TILE + q * HEAD, HEAD), HEAD)] = o.astype(BF16)

    def heads(s, g):
        e = HEAD**-0.5 * LOG2E
        half = m // 2
        at = lambda c: pl.ds(pl.multiple_of(d + c, HEAD), HEAD)
        for qb in range(2):
            keys, these = (qb + 1) * half, pl.ds(qb * half, half)
            kk, vv = hid[0:keys, at(2 * UNIT + g * HEAD)], hid[0:keys, at(3 * UNIT + g * HEAD)]
            q = jnp.concatenate([hid[these, at(2 * g * HEAD)], hid[these, at((2 * g + 1) * HEAD)]], axis=0)
            sc = lax.dot_general(kk, q, (((1,), (1,)), ((), ())), preferred_element_type=F32)
            ok = lax.broadcasted_iota(jnp.int32, (half, 2 * half), 0) <= lax.rem(lax.broadcasted_iota(jnp.int32, (half, 2 * half), 1), half)
            cut = jnp.where(ok, sc[qb * half :], HIDDEN)
            sc = cut if qb == 0 else jnp.concatenate([sc[:half], cut], axis=0)
            w = jnp.exp2((sc - sc.max(axis=0, keepdims=True)) * e).astype(BF16)
            mix = dot(jnp.concatenate([vv.T, jnp.ones((8, keys), BF16)], axis=0), w)
            o = (mix[:HEAD] * (1 / mix[HEAD : HEAD + 1])).T.astype(BF16)
            to = pl.ds(pl.multiple_of(s * m + qb * half, 16), half)
            for h in range(2):
                seen[to, pl.ds(pl.multiple_of((2 * g + h) * HEAD, HEAD), HEAD)] = o[h * half : (h + 1) * half]

    def first_service(k, first):
        here = lambda step: step % 8 // 4 == first

        for step, units in RELAYED.items():
            if here(step):
                @pl.when(k == step)
                def _():
                    for j in units:
                        received(rs1(j))
                        stage2(j)
                        start(rs2(j))

        for step, units in FINISHED.items():
            if here(step):
                @pl.when(k == step)
                def _():
                    for j in units:
                        received(rs2(j))
                        sent(rs1(j) + rs2(j))
                        stage3(j, 2, 0)
                        give_credit(j)

        if here(NORMED):
            @pl.when(k == NORMED)
            def _():
                h_norm(0)

    def attention(s, first):
        x_load(s).wait()
        if first:
            for i in range(4):
                start(qkv_tiles(i))
            x_block(0).start()
            for j in range(2):
                wo_unit(j).start()
        norm_rows(hid.at[:, pl.ds(0, d)], gains.at[0:1], b, m)

        @pl.when(s < last)
        def _():
            x_load(s + 1).start()

        @pl.loop(0, 4)
        def _(i):
            if first:
                for this in range(4):
                    @pl.when(i == this)
                    def _():
                        wait(qkv_tiles(this))
            else:
                first_service(8 * (s - 1) + i, 0)
            project(i)

        if not first:
            @pl.when(s == last)
            def _():
                start(gu_tiles(0, 0))

        @pl.loop(0, 4)
        def _(g):
            if not first:
                first_service(8 * (s - 1) + 4 + g, 1)
            heads(s, g)

    def burst(c):
        @pl.loop(0, nu)
        def _(j):
            par = lax.rem(j, 2)
            wo_unit(j).wait()
            out[par] = dot(seen[c * m : (c + 1) * m, :], wob[par])

            @pl.when(j < nu - 2)
            def _():
                wo_unit(j + 2).start()

            stage1(j, par)
            if c > 0:
                take_credit(j)
            start(rs1(j))

    barrier = pltpu.get_barrier_semaphore()
    for to in (left, right):
        pl.semaphore_signal(barrier, inc=1, device_id={"tp": to}, device_id_type=MESH)
    x_load(0).start()
    pl.semaphore_wait(barrier, 2)

    attention(0, True)
    x_block(0).wait()
    burst(0)
    for j in range(2):
        wo_unit(j).start()

    @pl.loop(1, seqs)
    def _(s):
        attention(s, False)

    for p in range(pieces):
        h_forward(0, p)
    burst(1)
    for j in range(2):
        wo_unit(j).start()
    sent(h_gather1(0))
    b_own(0).wait()
    received(h_gather2(0))
    sent(h_gather2(0))
    b_load(0).start()

    def pick(*units):
        there, second, c, j = units[0]
        for other in units[1:]:
            there, second, c, j = there | other[0], jnp.where(other[0], other[1], second), jnp.where(other[0], other[2], c), jnp.where(other[0], other[3], j)
        return there, second, c, j

    def span(cond, second, c, j):
        return cond & (j >= 0) & (j < nu), second, c, j

    def by_chunk(c, name):
        return jnp.where(c == 0, FIRST[name], TIMES[name]) if name in FIRST else TIMES[name]

    def gu_units(c, k):
        def pair(at, cond, sub):
            return span(cond & (k >= at), False, c + 1, 2 * (k - at) + sub)

        more = c < last
        one = [pair(TIMES["w"], more & (c > 0), sub) for sub in range(2)]
        two = [pair(by_chunk(c, "relay"), more, sub) for sub in range(2)]
        three = [pair(by_chunk(c, "finish"), more, sub) for sub in range(2)]
        one[0] = pick(one[0], span((c > 0) & (k == 0), True, c - 1, nu - 1 + 0 * k))
        two[0] = pick(two[0], span(c > 0, True, c - 1, k + nu - 1 - LAGS[0]))
        three[0] = pick(three[0], span(c > 0, True, c - 1, k + nu - 1 - LAGS[1]))
        return one, two, three

    def dn_units(c, j):
        final = c == last
        lag2, lag3 = (jnp.where(final, b_, a_) for a_, b_ in zip(LAGS, LAST_LAGS))
        return [span(True, True, c, j - 1)], [span(True, True, c, j - 1 - lag2)], [span(True, True, c, j - 1 - lag3)]

    def before(two, three):
        for there, _, _, j in two:
            @pl.when(there)
            def _():
                received(rs1(j))

        for there, second, _, j in three:
            @pl.when(there & jnp.logical_not(second) & (j == 0))
            def _():
                x_block(0).wait()

            @pl.when(there)
            def _():
                received(rs2(j))
                sent(rs1(j) + rs2(j))

    def math(one, two, three, par):
        place = lambda u: jnp.where(u[0], u[3], nu)
        for u in three:
            stage3(place(u), jnp.where(u[1], lax.rem(u[2], 2), 2), jnp.where(u[1], 3, lax.rem(u[2], 2)))
        for u in two:
            stage2(place(u))
        for sub, u in enumerate(one):
            stage1(place(u), sub if par is None else par)

    def after(one, two, three):
        for there, second, c, j in three:
            @pl.when(there)
            def _():
                give_credit(j)

            @pl.when(there & second)
            def _():
                y_block(c, j).start()

            @pl.when(there & second & (c == last))
            def _():
                start(y_gather1(c, j, bst))

        for there, _, _, j in two:
            @pl.when(there)
            def _():
                start(rs2(j))

        for there, _, _, j in one:
            @pl.when(there)
            def _():
                take_credit(j)
                start(rs1(j))

    def gathers(c, k, low, high):
        def at(tick, cond=True):
            return pl.when((k == tick) & cond) if low <= tick < high else lambda f: None

        def at_name(name, cond, part=None, add=0):
            a, b_ = (t[name] if part is None else t[name][part] for t in (FIRST, TIMES))
            if not (low <= a + add < high or low <= b_ + add < high):
                return lambda f: None
            return pl.when((k == jnp.where(c == 0, a, b_) + add) & cond)

        more = c < last

        @at(0, more)
        def _():
            x_block(c + 1).start()

        @at(LAGS[1] - nu + 1 + nu + 1, c > 0)
        def _():
            for j in range(nu):
                y_block(c - 1, j).wait()

        @at_name("norm", more)
        def _():
            h_norm(c + 1)

        for p in range(pieces):
            @at_name("forward", more, p)
            def _():
                h_forward(c + 1, p)

        @at_name("forward", more, pieces - 1, 1)
        def _():
            sent(h_gather1(c + 1))
            b_own(c + 1).wait()

        @at(per - 2, more)
        def _():
            received(h_gather2(c + 1))
            sent(h_gather2(c + 1))
            b_load(c + 1).start()

        @at(per - 2, (c > 0) & (c + 1 < last))
        def _():
            for j in range(2):
                wo_unit(j).start()

        for cy, (begin, stride) in enumerate(GATHER[:last]):
            since = c * per + k - (cy + 1) * per - begin
            for late, step in ((0, lambda j: start(y_gather1(cy, j))), (GATHER_LAG, lambda j: forward_y(cy, j))):
                i = jnp.maximum(since - late, 0)

                @pl.when((since >= late) & (lax.rem(i, stride) == 0) & (lax.div(i, stride) < nu))
                def _():
                    step(lax.div(i, stride))

    def forward_y(c, j):
        received(y_gather1(c, j))
        start(y_gather2(c, j))

    @pl.loop(0, seqs)
    def _(c):
        b_load(c).wait()

        def gate_up(low, high, counts, k):
            p = lax.rem(c * per + k, 2)
            wait(gu_tiles(0, p))

            @pl.when(k < ng - 1)
            def _():
                start(gu_tiles(k + 1, 1 - p))

            @pl.when(k == ng - 1)
            def _():
                start(dn_tiles(0, 1 - p))

            units = one, two, three = [u[:count] for u, count in zip(gu_units(c, k), counts)]
            for sub, (there, second, _, j) in enumerate(one):
                @pl.when(there & jnp.logical_not(second))
                def _():
                    wo_unit(sub).wait()
                    out[sub] = dot(seen[pl.ds(pl.multiple_of((c + 1) * m, 16), m), :], wob[sub])

                    @pl.when(j < nu - 2)
                    def _():
                        wo_unit(j + 2).start()

            before(two, three)
            for u in range(2):
                gate, up = dot(b[...], slot[p, u, :d]), dot(b[...], slot[p, u, d:])
                hid[:, pl.ds(pl.multiple_of(k * UNIT + u * TILE, TILE), TILE)] = (gate * jax.nn.sigmoid(gate) * up).astype(BF16)
            math(*units, None)
            after(*units)
            gathers(c, k, low, high)

        for low, high, counts in SEGMENTS:
            high = ng if high is None else high
            pl.loop(low, high)(functools.partial(gate_up, low, high, counts))

        @pl.loop(0, nu)
        def _(j):
            k = ng + j
            p = lax.rem(c * per + k, 2)
            wait(dn_tiles(0, p))

            @pl.when(j < nu - 1)
            def _():
                start(dn_tiles(j + 1, 1 - p))

            @pl.when((j == nu - 1) & (c < last))
            def _():
                start(gu_tiles(0, 1 - p))

            units = one, two, three = dn_units(c, j)
            before(two, three)
            for u in range(2):
                out[lax.rem(j, 2), :, u * TILE : (u + 1) * TILE] = dot(hid[...], slot[p, u])
            math(*units, lax.rem(j + 1, 2))
            after(*units)
            gathers(c, k, ng, per)

    stage1(nu - 1, (nu - 1) % 2)
    take_credit(nu - 1)
    start(rs1(nu - 1))
    relayed, finished = nu - 1 - LAST_LAGS[0], nu - 1 - LAST_LAGS[1]
    while finished < nu:
        if relayed < nu:
            received(rs1(relayed))
            stage2(relayed)
            start(rs2(relayed))
            relayed += 1
        while finished < min(relayed - 1, nu) or (relayed == nu and finished < nu):
            j = finished
            received(rs2(j))
            sent(rs1(j) + rs2(j))
            stage3(j, last % 2, 3)
            give_credit(j)
            y_block(last, j).start()
            start(y_gather1(last, j, bst))
            finished += 1
    for j in range(nu):
        forward_y(last, j)
    for j in range(nu):
        y_block(last, j).wait()
        take_credit(j)

    @pl.loop(0, seqs)
    def _(c):
        @pl.loop(0, nu)
        def _(j):
            sent(y_gather1(c, j) + y_gather2(c, j))
            received(y_gather2(c, j))


def rotary(rows):
    half = HEAD // 2
    angle = np.arange(rows, dtype=np.float32)[:, None] * np.float32(THETA) ** (-np.arange(half, dtype=np.float32) / half)
    cos, sin = np.cos(angle), np.sin(angle)
    return np.concatenate([cos, cos], -1), np.concatenate([-sin, sin], -1)


def solution(mesh):
    pieces = 3

    def step(x, gain_a, wq, wk, wv, wo, gain_m, w_gate, w_up, w_down):
        seqs, m, d = x.shape
        f, hq = w_gate.shape[1], wq.shape[1]
        blk, nu = m // 4, d // UNIT
        cos, sin = rotary(m)
        anywhere, vmem = pl.BlockSpec(memory_space=pl.ANY), pl.BlockSpec(memory_space=pltpu.VMEM)
        dma, V = pltpu.SemaphoreType.DMA, pltpu.VMEM
        y, _ = pl.pallas_call(
            functools.partial(layer_kernel, seqs, pieces),
            out_shape=[jax.ShapeDtypeStruct((seqs * m, d), BF16)] * 2,
            in_specs=[anywhere] + [vmem] * 3 + [anywhere] * 7,
            out_specs=[anywhere] * 2,
            scratch_shapes=[
                V((m, d), BF16), V((m, f), BF16), V((2, 2, 2 * d, TILE), BF16), V((seqs * m, hq), BF16), V((2, m, UNIT), F32),
                V((nu + 1, blk, UNIT), F32), V((2, nu + 1, blk, TILE), F32),
                V((2, nu + 1, 2, blk, TILE), BF16), V((2, nu + 1, blk, TILE), BF16),
                V((2, nu + 1, 2, blk, TILE), BF16), V((2, nu + 1, blk, TILE), BF16),
                V((4, blk, d + UNIT), BF16), V((2, hq, UNIT), BF16),
                dma((2, 4)), dma((2,)), dma, dma, dma, dma((2, nu)), dma((2, nu)), dma((2, nu)), dma((2, nu)),
                pltpu.SemaphoreType.REGULAR((2, nu)), dma((nu,)), dma,
                dma((2, pieces)), dma((2, pieces)), dma((2, pieces)), dma((2, pieces)),
                *[dma((seqs, 2, nu))] * 4,
            ],
            compiler_params=pltpu.CompilerParams(collective_id=0, has_side_effects=True, vmem_limit_bytes=67043328),
            name="layer",
        )(x.reshape(seqs * m, d), cos, sin, jnp.stack([gain_a, gain_m]), wq, wk, wv, wo, w_gate, w_up, w_down)
        return y.reshape(x.shape)

    tokens, whole, columns, rows_of = P("dp", None, None), P(None), P(None, "tp"), P("tp", None)
    return jax.shard_map(
        step,
        mesh=mesh,
        in_specs=(tokens, whole, columns, columns, columns, rows_of, whole, columns, columns, rows_of),
        out_specs=tokens,
        check_vma=False,
    )
```
